32 devices in a mesh: rows: 8 (over z, x), grp: 4 (over y, core).
Axes of the slice: x: 2, y: 2, z: 4, core: 2. Of those that a mesh axis runs over, the one named last changes fastest.
Arguments:
- matrix: bfloat16 [10240, 16384], P(('rows', 'grp')), may hold values from -36 to 36
- sample_rows: int32 [32, 128, 256], P(('rows', 'grp')), may hold values from 0 to 319
- pair_list: int32 [8, 8, 4], replicated, may hold values from 0 to 255, as said below
- pair_count: int32 [8, 8], replicated, may hold values from 1 to 4, as said below
- pair_blocks: int32 [256, 2], replicated, may hold values from 0 to 127, as said below
Outputs:
- gram: float32 [256, 128, 128], P(('rows', 'grp'))
The draws below stay inside these ranges and needn't reach their ends.
Inputs may be any that keep to these rules, and one draw needn't show every extreme that they name: `pair_list`: entry [s, r, k] lies in [r * 32, (r + 1) * 32); the 4 entries of one [s, r] are distinct. `pair_count`: every row group has some owner with all 4 slots active, and some owner has all 4 slots active from every row group. `pair_blocks`: the two blocks of a pair differ.
All inputs are finite; a program needn't handle non-finite values.
Results may differ from the reference program's by a relative error of at most 0.0016.
Values sent between devices are 32-bit elements; how exact they have to be, the bound alone decides.
No kernel may reach another device: no remote copies, remote signals or barrier semaphores. Data moves between devices by JAX's collectives and lax.ppermute only.
A program may use at most 192 MiB of HBM per device.

```python
import math
import jax
import jax.numpy as jnp
from jax import lax

BLOCK = 128
NB = 128
ROWS_DEV = 320
SAMP = 256
CAP = 4
NCOL = 16384
ROWS_TOTAL = 10240
PAIRS = 256
REGION = 32
N_ROWS = 8
N_GRP = 4
DEVICES = 32


def draw_matrix(key, part):
    key_base, key_row, key_col = jax.random.split(key, 3)
    row_scale = jnp.exp(jax.random.uniform(key_row, (ROWS_TOTAL, 1), jnp.float32, math.log(0.3), math.log(3.0)))
    col_scale = jnp.exp(jax.random.uniform(key_col, (1, NCOL), jnp.float32, math.log(0.5), math.log(2.0)))
    base = jnp.clip(jax.random.normal(key_base, (ROWS_TOTAL, NCOL), jnp.float32), -6.0, 6.0)
    return (base * row_scale * col_scale).astype(jnp.bfloat16)


def draw_pair_list(key, part):
    keys = jax.random.split(jax.random.fold_in(key, 11), N_ROWS * N_ROWS)
    chosen = jax.vmap(lambda single: jax.random.permutation(single, REGION)[:CAP])(keys)
    chosen = chosen.reshape(N_ROWS, N_ROWS, CAP).astype(jnp.int32)
    owner_base = (jnp.arange(N_ROWS, dtype=jnp.int32) * REGION)[None, :, None]
    return chosen + owner_base


def draw_pair_count(key, part):
    key_count, key_row, key_col = jax.random.split(jax.random.fold_in(key, 23), 3)
    counts = jax.random.randint(key_count, (N_ROWS, N_ROWS), 1, CAP + 1).astype(jnp.int32)
    full_owner = jax.random.randint(key_row, (N_ROWS,), 0, N_ROWS)
    counts = counts.at[jnp.arange(N_ROWS), full_owner].set(CAP)
    common_owner = jax.random.randint(key_col, (), 0, N_ROWS)
    counts = counts.at[:, common_owner].set(CAP)
    return counts.astype(jnp.int32)


def draw_pair_blocks(key, part):
    key_first, key_step = jax.random.split(jax.random.fold_in(key, 37))
    first_block = jax.random.randint(key_first, (PAIRS,), 0, NB)
    step_size = jax.random.randint(key_step, (PAIRS,), 1, NB)
    second_block = (first_block + step_size) % NB
    return jnp.stack([first_block, second_block], axis=1).astype(jnp.int32)


def touch_ends(result, rng, smallest, high):
    dims = result.shape
    place = [jax.random.randint(jax.random.fold_in(rng, axis), (), 0, dims[axis]) for axis in range(len(dims))]
    result = result.at[tuple(place)].set(smallest)
    longest = dims.index(max(dims))
    place[longest] = (place[longest] + 1) % dims[longest]
    return result.at[tuple(place)].set(high)


def setup_inputs(seed: int = 0) -> dict:
    seeds = jax.random.split(jax.random.key(seed), 6)
    return {
        "matrix": draw_matrix(jax.random.fold_in(seeds[5], 71), 0),
        "sample_rows": touch_ends(jax.random.randint(seeds[1], (DEVICES, NB, SAMP), 0, ROWS_DEV), jax.random.fold_in(seeds[1], 1), 0, ROWS_DEV - 1).astype(jnp.int32),
        "pair_list": draw_pair_list(jax.random.fold_in(seeds[5], 71), 0),
        "pair_count": draw_pair_count(jax.random.fold_in(seeds[5], 71), 0),
        "pair_blocks": draw_pair_blocks(jax.random.fold_in(seeds[5], 71), 0),
    }


def reference(matrix, sample_rows, pair_list, pair_count, pair_blocks):
    device_total = N_ROWS * N_GRP
    blocks_all = matrix.reshape(device_total, ROWS_DEV, NB, BLOCK)
    positions = jnp.arange(ROWS_DEV, dtype=jnp.int32)
    slot_numbers = jnp.arange(CAP, dtype=jnp.int32)

    def one_device(raw_tiles, device):
        source = device // N_GRP
        blocks = blocks_all[device]
        picked = sample_rows[device]
        multiplicity = lax.optimization_barrier(jnp.sum((picked[:, :, None] == positions[None, None, :]).astype(jnp.float32), axis=1))
        weighted = (jnp.transpose(multiplicity)[:, :, None] * blocks.astype(jnp.float32)).astype(jnp.bfloat16)
        pair_ids = pair_list[source].reshape(-1)
        live_mask = (slot_numbers[None, :] < pair_count[source][:, None]).reshape(-1).astype(jnp.float32)
        first_block = pair_blocks[pair_ids, 0]
        second_block = pair_blocks[pair_ids, 1]
        weighted_cols = jnp.take(weighted, first_block, axis=1).astype(jnp.float32)
        plain_cols = jnp.take(blocks, second_block, axis=1).astype(jnp.float32)
        partial_tiles = jnp.einsum('rgi,rgj->gij', weighted_cols, plain_cols)
        partial_tiles = partial_tiles * live_mask[:, None, None]
        return (raw_tiles.at[pair_ids].add(partial_tiles), None)
    start = jnp.zeros((PAIRS, BLOCK, BLOCK), jnp.float32)
    raw_tiles, _ = lax.scan(one_device, start, jnp.arange(device_total, dtype=jnp.int32))
    squares = lax.optimization_barrier(jnp.sum(jnp.square(matrix.astype(jnp.float32)), axis=0))
    root_mean = jnp.sqrt(squares / ROWS_TOTAL + 1e-06).reshape(NB, BLOCK)
    left_scale = root_mean[pair_blocks[:, 0]]
    right_scale = root_mean[pair_blocks[:, 1]]
    return raw_tiles / (SAMP * left_scale[:, :, None] * right_scale[:, None, :])
```

```python
import functools

import jax
import jax.numpy as jnp
from jax import lax
from jax.experimental import pallas as pl
from jax.experimental.pallas import tpu as pltpu
from jax.sharding import PartitionSpec as P

epsilon = 1e-06


class Dims:
    def __init__(self, mesh, matrix, sample_rows, pair_list, pair_blocks):
        self.rows_axis = mesh.shape["rows"]
        self.grp_axis = mesh.shape["grp"]
        self.rows_dev, self.columns = matrix.shape
        self.blocks = sample_rows.shape[1]
        self.samples = sample_rows.shape[2]
        self.width = self.columns // self.blocks
        self.cap = pair_list.shape[2]
        self.pairs = pair_blocks.shape[0]
        self.region = self.pairs // self.rows_axis
        self.own = self.region // self.grp_axis
        self.part = self.width // self.grp_axis
        self.rows_total = self.rows_dev * self.rows_axis * self.grp_axis
        self.tile_rows = self.cap * self.part
        self.message = self.tile_rows + 2 * self.own
        self.count_at = self.rows_axis * self.rows_axis * self.cap
        self.block_at = self.count_at + self.rows_axis * self.rows_axis


def tiles_kernel(n, table, samples, matrix, *rest):
    outs = rest[: n.grp_axis]
    local, sums, tile, arrive = rest[n.grp_axis :]
    me = lax.axis_index("rows")
    g = lax.axis_index("grp")
    pieces = arrive.shape[0]
    piece_blocks = n.blocks // pieces
    piece = piece_blocks * n.width

    def copy(i):
        span = pl.ds(i * piece, piece)
        return pltpu.make_async_copy(matrix.at[:, span], local.at[:, span], arrive.at[i])

    for i in range(pieces):
        copy(i).start()

    def block_sum(b, carry):
        x = local[:, pl.ds(pl.multiple_of(b * n.width, n.width), n.width)].astype(jnp.float32)
        sums[pl.ds(b, 1), :] = jnp.sum(x * x, axis=0, keepdims=True)
        return carry

    for i in range(pieces):
        copy(i).wait()
        lax.fori_loop(i * piece_blocks, (i + 1) * piece_blocks, block_sum, 0, unroll=2)

    for d in range(n.grp_axis):

        def place(o, carry, d=d):
            first = (jnp.bitwise_xor(o, me) * n.grp_axis + jnp.bitwise_xor(g, d)) * n.own
            for j in range(n.own):
                for side in range(2):
                    b = table[n.block_at + 2 * (first + j) + side]
                    outs[d][o, pl.ds(n.tile_rows + 2 * j + side, 1), :] = sums[pl.ds(b, 1), :]
            return carry

        lax.fori_loop(0, n.rows_axis, place, 0)

    positions = lax.broadcasted_iota(jnp.int32, (n.rows_dev, n.samples), 0)
    ones = jnp.ones((n.samples, n.width), jnp.bfloat16)

    def slot(t, carry):
        o = t // n.cap
        k = t % n.cap
        at = me * n.rows_axis + jnp.bitwise_xor(o, me)
        live = k < table[n.count_at + at]
        row = pl.multiple_of(k * n.part, n.part)

        @pl.when(live)
        def _():
            pair = table[at * n.cap + k]
            b = table[n.block_at + 2 * pair]
            c = table[n.block_at + 2 * pair + 1]
            drawn = samples[0, pl.ds(b, 1), :]
            hit = jnp.where(drawn == positions, 1.0, 0.0).astype(jnp.bfloat16)
            times = jnp.dot(hit, ones, preferred_element_type=jnp.float32)
            left = local[:, pl.ds(pl.multiple_of(b * n.width, n.width), n.width)]
            right = local[:, pl.ds(pl.multiple_of(c * n.width, n.width), n.width)]
            weighted = (times * left.astype(jnp.float32)).astype(jnp.bfloat16)
            tile[...] = lax.dot_general(
                weighted, right, (((0,), (0,)), ((), ())), preferred_element_type=jnp.float32
            )

        @pl.when(jnp.logical_not(live))
        def _():
            tile[...] = jnp.zeros_like(tile)

        for d in range(n.grp_axis):
            q = pl.multiple_of(jnp.bitwise_xor(g, d) * n.part, n.part)
            outs[d][o, pl.ds(row, n.part), :] = tile[pl.ds(q, n.part), :]
        return carry

    lax.fori_loop(0, n.rows_axis * n.cap, slot, 0)


def spread_kernel(n, *refs):
    a, b, c = refs[:3]
    outs = refs[3:]
    for o in range(n.rows_axis):
        outs[o][...] = a[o] + b[o] + c[o]


def gather_kernel(n, table, *refs):
    parts = refs[: n.rows_axis]
    outs = refs[n.rows_axis : n.rows_axis + n.grp_axis]
    total, acc = refs[n.rows_axis + n.grp_axis :]
    me = lax.axis_index("rows")
    g = lax.axis_index("grp")
    acc[...] = jnp.zeros_like(acc)
    column = jnp.zeros((2 * n.own, n.width), jnp.float32)
    for o in range(n.rows_axis):
        at = jnp.bitwise_xor(me, o) * n.rows_axis + me
        for k in range(n.cap):
            i = table[at * n.cap + k] - me * n.region
            acc[i] += parts[o][pl.ds(k * n.part, n.part), :]
        column = column + parts[o][pl.ds(n.tile_rows, 2 * n.own), :]
    total[...] = column
    for d in range(n.grp_axis):
        outs[d][...] = acc[pl.ds(jnp.bitwise_xor(g, d) * n.own, n.own)]


def scale_kernel(n, total, *refs):
    parts = refs[: n.grp_axis]
    out = refs[n.grp_axis]
    g = lax.axis_index("grp")
    root = jnp.sqrt(total[...] / n.rows_total + epsilon)
    for j in range(n.own):
        left = jnp.transpose(jnp.broadcast_to(root[2 * j : 2 * j + 1], (n.width, n.width)))
        out[j] = n.samples * left * root[2 * j + 1 : 2 * j + 2]
    for d in range(n.grp_axis):
        q = pl.multiple_of(jnp.bitwise_xor(g, d) * n.part, n.part)
        for j in range(n.own):
            out[j, pl.ds(q, n.part), :] = parts[d][j] / out[j, pl.ds(q, n.part), :]


def swap(n, x, axis, size, distance):
    return lax.ppermute(x, axis, [(i, i ^ distance) for i in range(size)])


def shards(mesh, matrix, sample_rows, pair_list, pair_count, pair_blocks):
    n = Dims(mesh, matrix, sample_rows, pair_list, pair_blocks)
    f32 = jnp.float32
    vmem = pl.BlockSpec(memory_space=pltpu.VMEM)
    smem = pl.BlockSpec(memory_space=pltpu.SMEM)
    table = jnp.concatenate([pair_list.reshape(-1), pair_count.reshape(-1), pair_blocks.reshape(-1)])
    pieces = 16
    message = jax.ShapeDtypeStruct((n.rows_axis, n.message, n.width), f32)
    sent = pl.pallas_call(
        functools.partial(tiles_kernel, n),
        out_shape=[message] * n.grp_axis,
        in_specs=[smem, vmem, pl.BlockSpec(memory_space=pl.ANY)],
        out_specs=[vmem] * n.grp_axis,
        scratch_shapes=[
            pltpu.VMEM(matrix.shape, matrix.dtype),
            pltpu.VMEM((n.blocks, n.width), f32),
            pltpu.VMEM((n.width, n.width), f32),
            pltpu.SemaphoreType.DMA((pieces,)),
        ],
        name="tiles",
    )(table, sample_rows, matrix)
    sent = list(sent)
    distance = 1
    extra = None
    while distance * 2 < n.grp_axis:
        came = {d: swap(n, sent[d], "grp", n.grp_axis, distance) for d in reversed(range(n.grp_axis)) if d & distance and d % (2 * distance) == distance}
        kept = [d for d in range(0, n.grp_axis, 2 * distance)]
        for d in kept:
            if d == 0:
                extra = came[distance]
            else:
                sent[d] = sent[d] + came[d + distance]
        distance *= 2
    last = swap(n, sent[distance], "grp", n.grp_axis, distance)
    one = jax.ShapeDtypeStruct((n.message, n.width), f32)
    spread = pl.pallas_call(
        functools.partial(spread_kernel, n),
        out_shape=[one] * n.rows_axis,
        in_specs=[vmem] * 3,
        out_specs=[vmem] * n.rows_axis,
        name="spread",
    )(sent[0], extra, last)
    came = [spread[0]] + [
        swap(n, spread[o], "rows", n.rows_axis, o) for o in range(1, n.rows_axis)
    ]
    quarter = jax.ShapeDtypeStruct((n.own, n.part, n.width), f32)
    *owned, total = pl.pallas_call(
        functools.partial(gather_kernel, n),
        out_shape=[quarter] * n.grp_axis + [jax.ShapeDtypeStruct((2 * n.own, n.width), f32)],
        in_specs=[smem] + [vmem] * n.rows_axis,
        out_specs=[vmem] * (n.grp_axis + 1),
        scratch_shapes=[pltpu.VMEM((n.region, n.part, n.width), f32)],
        name="gather",
    )(table, *came)
    came = [owned[0]] + [swap(n, owned[d], "grp", n.grp_axis, d) for d in range(1, n.grp_axis)]
    return pl.pallas_call(
        functools.partial(scale_kernel, n),
        out_shape=jax.ShapeDtypeStruct((n.own, n.width, n.width), f32),
        in_specs=[vmem] * (n.grp_axis + 1),
        out_specs=vmem,
        name="scale",
    )(total, *came)


def solution(mesh):
    in_specs = (P(("rows", "grp"), None), P(("rows", "grp"), None, None), P(), P(), P())
    out_specs = P(("rows", "grp"), None, None)
    return jax.shard_map(
        functools.partial(shards, mesh), mesh=mesh, in_specs=in_specs, out_specs=out_specs, check_vma=False
    )
```

```python
import functools

import jax
import jax.numpy as jnp
from jax import lax
from jax.experimental import pallas as pl
from jax.experimental.pallas import tpu as pltpu
from jax.sharding import PartitionSpec as P

epsilon = 1e-06
unroll = 4
pieces = 16
late_slots = 1


class Dims:
    def __init__(self, mesh, matrix, sample_rows, pair_list, pair_blocks):
        self.rows_axis = mesh.shape["rows"]
        self.grp_axis = mesh.shape["grp"]
        self.rows_dev, self.columns = matrix.shape
        self.blocks = sample_rows.shape[1]
        self.samples = sample_rows.shape[2]
        self.width = self.columns // self.blocks
        self.cap = pair_list.shape[2]
        self.pairs = pair_blocks.shape[0]
        self.region = self.pairs // self.rows_axis
        self.own = self.region // self.grp_axis
        self.part = self.width // self.grp_axis
        self.rows_total = self.rows_dev * self.rows_axis * self.grp_axis


def list_live(n, first, last, live, counts):
    me = lax.axis_index("rows")

    def scan(o, found):
        r = jnp.bitwise_xor(o, me)
        top = jnp.minimum(counts[me, r], last)

        def add(k, found):
            live[found] = o * n.cap + k
            return found + 1

        return lax.fori_loop(first, top, add, found)

    return lax.fori_loop(0, n.rows_axis, scan, 0)


def multiply(n, first, slots, loads, samples, blocks_of, stage, outs):
    g = lax.axis_index("grp")
    positions = lax.broadcasted_iota(jnp.int32, (n.rows_dev, n.samples), 0)
    ones = jnp.ones((n.samples, n.width), jnp.bfloat16)
    for u, t in enumerate(slots):
        drawn = samples[0, pl.ds(blocks_of(t)[0], 1), :]
        hit = jnp.where(drawn == positions, 1.0, 0.0).astype(jnp.bfloat16)
        times = jnp.dot(hit, ones, preferred_element_type=jnp.float32)
        left, right = loads(u, t)
        weighted = (times * left.astype(jnp.float32)).astype(jnp.bfloat16)
        stage[u] = lax.dot_general(
            weighted, right, (((0,), (0,)), ((), ())), preferred_element_type=jnp.float32
        )
    for u, t in enumerate(slots):
        o = t // n.cap
        row = pl.multiple_of((t % n.cap - first) * n.part, n.part)
        for d in range(n.grp_axis):
            q = pl.multiple_of(jnp.bitwise_xor(g, d) * n.part, n.part)
            outs[d][o, pl.ds(row, n.part), :] = stage[u, pl.ds(q, n.part), :]


def split_outs(n, refs):
    return [refs[0].at[d // 2] if d % 2 else refs[1 + d // 2] for d in range(n.grp_axis)]


def clear(outs, n, rows):
    zero = jnp.zeros((rows, n.width), jnp.float32)

    def body(o, carry):
        for out in outs:
            out[o, pl.ds(0, rows), :] = zero
        return carry

    lax.fori_loop(0, n.rows_axis, body, 0)


def early_kernel(n, last, lists, counts, pairs, samples, matrix, *rest):
    outs = split_outs(n, rest[: 1 + n.grp_axis // 2])
    held, stage, live, arrive = rest[1 + n.grp_axis // 2 :]
    me = lax.axis_index("rows")

    def blocks_of(t):
        pair = lists[me, t % n.cap, jnp.bitwise_xor(t // n.cap, me)]
        return pairs[0, pair], pairs[1, pair]

    def copies(i, t):
        both = blocks_of(t)
        return [
            pltpu.make_async_copy(
                matrix.at[:, pl.ds(pl.multiple_of(both[side] * n.width, n.width), n.width)],
                held.at[i, side],
                arrive.at[i],
            )
            for side in range(2)
        ]

    found = list_live(n, 0, last, live, counts)

    def begin(i, carry):
        for copy in copies(i, live[i]):
            copy.start()
        return carry

    lax.fori_loop(0, found, begin, 0)
    clear(outs, n, last * n.part)

    def group(i, carry):
        at = [jnp.where(i * unroll + u < found, i * unroll + u, 0) for u in range(unroll)]
        slots = [live[a] for a in at]
        for u in range(unroll):

            @pl.when(i * unroll + u < found)
            def _(u=u):
                for copy in copies(at[u], slots[u]):
                    copy.wait()

        def loads(u, t):
            return held[at[u], 0], held[at[u], 1]

        multiply(n, 0, slots, loads, samples, blocks_of, stage, outs)
        return carry

    lax.fori_loop(0, pl.cdiv(found, unroll), group, 0)


def late_kernel(n, first, lists, counts, pairs, samples, matrix, after, *rest):
    outs = split_outs(n, rest[: 1 + n.grp_axis // 2])
    local, sums, stage, live, arrive = rest[1 + n.grp_axis // 2 :]
    me = lax.axis_index("rows")
    g = lax.axis_index("grp")
    piece_blocks = n.blocks // pieces
    piece = piece_blocks * n.width
    tile_rows = (n.cap - first) * n.part

    def copy(i):
        span = pl.ds(i * piece, piece)
        return pltpu.make_async_copy(matrix.at[:, span], local.at[:, span], arrive.at[i])

    for i in range(pieces):
        copy(i).start()
    found = list_live(n, first, n.cap, live, counts)
    clear(outs, n, tile_rows)

    def columns(b):
        return local[:, pl.ds(pl.multiple_of(b * n.width, n.width), n.width)]

    def block_sum(b, carry):
        x = columns(b).astype(jnp.float32)
        sums[pl.ds(b, 1), :] = jnp.sum(x * x, axis=0, keepdims=True)
        return carry

    for i in range(pieces):
        copy(i).wait()
        lax.fori_loop(i * piece_blocks, (i + 1) * piece_blocks, block_sum, 0, unroll=2)

    for d in range(n.grp_axis):

        def place(o, carry, d=d):
            base = (jnp.bitwise_xor(o, me) * n.grp_axis + jnp.bitwise_xor(g, d)) * n.own
            for j in range(n.own):
                for side in range(2):
                    b = pairs[side, base + j]
                    outs[d][o, pl.ds(tile_rows + 2 * j + side, 1), :] = sums[pl.ds(b, 1), :]
            return carry

        lax.fori_loop(0, n.rows_axis, place, 0)

    def blocks_of(t):
        pair = lists[me, t % n.cap, jnp.bitwise_xor(t // n.cap, me)]
        return pairs[0, pair], pairs[1, pair]

    def group(i, carry):
        slots = [live[jnp.where(i * unroll + u < found, i * unroll + u, 0)] for u in range(unroll)]

        def loads(u, t):
            both = blocks_of(t)
            return columns(both[0]), columns(both[1])

        multiply(n, first, slots, loads, samples, blocks_of, stage, outs)
        return carry

    lax.fori_loop(0, pl.cdiv(found, unroll), group, 0)


def spread_kernel(n, *refs):
    halves = [refs[:3], refs[3:6]]
    outs = refs[6:]
    for o in range(n.rows_axis):
        at = 0
        for kept, core, chip in halves:
            rows = kept.shape[1]
            outs[o][pl.ds(at, rows), :] = kept[o] + core[0, o] + chip[o]
            at += rows


def gather_kernel(n, lists, *refs):
    parts = refs[: n.rows_axis]
    outs = refs[n.rows_axis : n.rows_axis + n.grp_axis]
    total, acc = refs[n.rows_axis + n.grp_axis :]
    me = lax.axis_index("rows")
    g = lax.axis_index("grp")
    acc[...] = jnp.zeros_like(acc)
    column = jnp.zeros((2 * n.own, n.width), jnp.float32)
    for o in range(n.rows_axis):
        source = jnp.bitwise_xor(me, o)
        for k in range(n.cap):
            i = lists[source, k, me] - me * n.region
            acc[i] += parts[o][pl.ds(k * n.part, n.part), :]
        column = column + parts[o][pl.ds(n.cap * n.part, 2 * n.own), :]
    total[...] = column
    for d in range(n.grp_axis):
        outs[d][...] = acc[pl.ds(jnp.bitwise_xor(g, d) * n.own, n.own)]


def factor_kernel(n, total, out):
    root = jnp.sqrt(total[...] / n.rows_total + epsilon)
    for j in range(n.own):
        left = jnp.transpose(jnp.broadcast_to(root[2 * j : 2 * j + 1], (n.width, n.width)))
        out[j] = 1.0 / (n.samples * left * root[2 * j + 1 : 2 * j + 2])


def scale_kernel(n, factor, *refs):
    parts = refs[: n.grp_axis]
    out = refs[n.grp_axis]
    g = lax.axis_index("grp")
    for d in range(n.grp_axis):
        q = pl.ds(pl.multiple_of(jnp.bitwise_xor(g, d) * n.part, n.part), n.part)
        for j in range(n.own):
            out[j, q, :] = parts[d][j] * factor[j, q, :]


def swap(x, axis, size, distance):
    return lax.ppermute(x, axis, [(i, i ^ distance) for i in range(size)])


def megabytes(*shapes):
    total = sum(4 * functools.reduce(lambda a, b: a * b, s) for s in shapes)
    return pltpu.CompilerParams(vmem_limit_bytes=int(total) + (2 << 20))


def shards(mesh, matrix, sample_rows, pair_list, pair_count, pair_blocks):
    n = Dims(mesh, matrix, sample_rows, pair_list, pair_blocks)
    f32 = jnp.float32
    vmem = pl.BlockSpec(memory_space=pltpu.VMEM)
    smem = pl.BlockSpec(memory_space=pltpu.SMEM)
    hbm = pl.BlockSpec(memory_space=pl.ANY)
    matrix = pltpu.with_memory_space_constraint(matrix, pltpu.HBM)
    lists = jnp.transpose(pair_list, (0, 2, 1))
    pairs = jnp.transpose(pair_blocks)
    half = n.grp_axis // 2
    first = n.cap - late_slots

    def stage_outs(rows):
        one = (n.rows_axis, rows, n.width)
        return [jax.ShapeDtypeStruct((half,) + one, f32)] + [jax.ShapeDtypeStruct(one, f32)] * half

    stage = (unroll, n.width, n.width)
    slots = n.rows_axis * first
    rows = first * n.part
    early = pl.pallas_call(
        functools.partial(early_kernel, n, first),
        out_shape=stage_outs(rows),
        in_specs=[smem, smem, smem, vmem, hbm],
        out_specs=[vmem] * (1 + half),
        scratch_shapes=[
            pltpu.VMEM((slots, 2, n.rows_dev, n.width), matrix.dtype),
            pltpu.VMEM(stage, f32),
            pltpu.SMEM((slots,), jnp.int32),
            pltpu.SemaphoreType.DMA((slots,)),
        ],
        compiler_params=megabytes(
            (slots, n.rows_dev, n.width), stage, sample_rows.shape, (n.grp_axis, n.rows_axis, rows, n.width)
        ),
        name="early_tiles",
    )(lists, pair_count, pairs, sample_rows, matrix)

    def reduce_scatter(outs):
        got = swap(outs[0], "grp", n.grp_axis, 1)
        kept = {2 * i: outs[1 + i] + got[i] for i in range(1, half)}
        sent = kept[half]
        result = [outs[1], got]
        distance = 2
        while distance < n.grp_axis:
            came = {d: swap(kept[d], "grp", n.grp_axis, distance) for d in kept if d & distance}
            result.append(came.pop(distance))
            kept = {d: kept[d] + came[d + distance] for d in kept if not d & distance}
            distance *= 2
        chips = result[2]
        for more in result[3:]:
            chips = chips + more
        return [outs[1], got, chips], sent

    early_sums, sent = reduce_scatter(early)
    late_rows = late_slots * n.part + 2 * n.own
    slots = n.rows_axis * late_slots
    late = pl.pallas_call(
        functools.partial(late_kernel, n, first),
        out_shape=stage_outs(late_rows),
        in_specs=[smem, smem, smem, vmem, hbm, hbm],
        out_specs=[vmem] * (1 + half),
        scratch_shapes=[
            pltpu.VMEM(matrix.shape, matrix.dtype),
            pltpu.VMEM((n.blocks, n.width), f32),
            pltpu.VMEM(stage, f32),
            pltpu.SMEM((slots,), jnp.int32),
            pltpu.SemaphoreType.DMA((pieces,)),
        ],
        compiler_params=megabytes(
            (n.rows_dev, n.columns // 2), stage, sample_rows.shape, (n.grp_axis, n.rows_axis, late_rows, n.width)
        ),
        cost_estimate=pl.CostEstimate(
            flops=2 * slots * n.rows_dev * n.width * (n.width + n.samples) + 3 * matrix.size,
            transcendentals=0,
            bytes_accessed=2 * matrix.size,
        ),
        name="late_tiles",
    )(lists, pair_count, pairs, sample_rows, matrix, sent)

    halves = early_sums + reduce_scatter(late)[0]
    message = (n.cap * n.part + 2 * n.own, n.width)
    small = megabytes((4 * n.rows_axis,) + message)
    spread = pl.pallas_call(
        functools.partial(spread_kernel, n),
        out_shape=[jax.ShapeDtypeStruct(message, f32)] * n.rows_axis,
        in_specs=[vmem] * 6,
        out_specs=[vmem] * n.rows_axis,
        compiler_params=small,
        name="spread",
    )(*halves)
    came = [spread[0]] + [swap(spread[o], "rows", n.rows_axis, o) for o in range(1, n.rows_axis)]
    quarter = (n.own, n.part, n.width)
    *owned, total = pl.pallas_call(
        functools.partial(gather_kernel, n),
        out_shape=[jax.ShapeDtypeStruct(quarter, f32)] * n.grp_axis
        + [jax.ShapeDtypeStruct((2 * n.own, n.width), f32)],
        in_specs=[smem] + [vmem] * n.rows_axis,
        out_specs=[vmem] * (n.grp_axis + 1),
        scratch_shapes=[pltpu.VMEM((n.region, n.part, n.width), f32)],
        compiler_params=megabytes((n.rows_axis,) + message, (2 * n.grp_axis,) + quarter),
        name="gather",
    )(lists, *came)
    came = [owned[0]] + [
        swap(owned[d], "grp", n.grp_axis, d) for d in reversed(range(1, n.grp_axis))
    ][::-1]
    tiles = (n.own, n.width, n.width)
    factor = pl.pallas_call(
        functools.partial(factor_kernel, n),
        out_shape=jax.ShapeDtypeStruct(tiles, f32),
        in_specs=[vmem],
        out_specs=vmem,
        compiler_params=megabytes(tiles),
        name="factor",
    )(total)
    return pl.pallas_call(
        functools.partial(scale_kernel, n),
        out_shape=jax.ShapeDtypeStruct(tiles, f32),
        in_specs=[vmem] * (n.grp_axis + 1),
        out_specs=vmem,
        compiler_params=megabytes(tiles, tiles, tiles),
        name="scale",
    )(factor, *came)


def solution(mesh):
    in_specs = (P(("rows", "grp"), None), P(("rows", "grp"), None, None), P(), P(), P())
    out_specs = P(("rows", "grp"), None, None)

    def body(*args):
        return shards(mesh, *args)

    return jax.shard_map(body, mesh=mesh, in_specs=in_specs, out_specs=out_specs, check_vma=False)
```

```python
import functools

import jax
import jax.numpy as jnp
from jax import lax
from jax.experimental import pallas as pl
from jax.experimental.pallas import tpu as pltpu
from jax.sharding import PartitionSpec as P

epsilon = 1e-06
unroll = 4
late_slots = 1


class Dims:
    def __init__(self, mesh, matrix, sample_rows, pair_list, pair_blocks):
        self.rows_axis = mesh.shape["rows"]
        self.grp_axis = mesh.shape["grp"]
        self.rows_dev, self.columns = matrix.shape
        self.blocks = sample_rows.shape[1]
        self.samples = sample_rows.shape[2]
        self.width = self.columns // self.blocks
        self.cap = pair_list.shape[2]
        self.pairs = pair_blocks.shape[0]
        self.region = self.pairs // self.rows_axis
        self.own = self.region // self.grp_axis
        self.part = self.width // self.grp_axis
        self.rows_total = self.rows_dev * self.rows_axis * self.grp_axis


def list_live(n, first, last, live, counts):
    me = lax.axis_index("rows")

    def scan(o, found):
        r = jnp.bitwise_xor(o, me)
        top = jnp.minimum(counts[me, r], last)

        def add(k, found):
            live[found] = o * n.cap + k
            return found + 1

        return lax.fori_loop(first, top, add, found)

    return lax.fori_loop(0, n.rows_axis, scan, 0)


def multiply(n, first, slots, loads, samples, blocks_of, stage, outs):
    g = lax.axis_index("grp")
    positions = lax.broadcasted_iota(jnp.int32, (n.rows_dev, n.samples), 0)
    for u, t in enumerate(slots):
        drawn = samples[pl.ds(blocks_of(t)[0], 1), :]
        times = jnp.sum(jnp.where(drawn == positions, 1.0, 0.0), axis=1, keepdims=True)
        left, right = loads(u, t)
        weighted = (times * left.astype(jnp.float32)).astype(jnp.bfloat16)
        stage[u] = lax.dot_general(
            weighted, right, (((0,), (0,)), ((), ())), preferred_element_type=jnp.float32
        )
    for u, t in enumerate(slots):
        o = t // n.cap
        row = pl.multiple_of((t % n.cap - first) * n.part, n.part)
        for d in range(n.grp_axis):
            q = pl.multiple_of(jnp.bitwise_xor(g, d) * n.part, n.part)
            outs[d][o, pl.ds(row, n.part), :] = stage[u, pl.ds(q, n.part), :]


def split_outs(n, refs):
    return [refs[0].at[d // 2] if d % 2 else refs[1 + d // 2] for d in range(n.grp_axis)]


def clear(outs, n, rows):
    zero = jnp.zeros((rows, n.width), jnp.float32)

    def body(o, carry):
        for out in outs:
            out[o, pl.ds(0, rows), :] = zero
        return carry

    lax.fori_loop(0, n.rows_axis, body, 0)


def early_kernel(n, last, lists, counts, pairs, samples, matrix, *rest):
    outs = split_outs(n, rest[: 1 + n.grp_axis // 2])
    held, drawn, stage, live, arrive, came = rest[1 + n.grp_axis // 2 :]
    me = lax.axis_index("rows")
    draws = pltpu.make_async_copy(samples.at[0], drawn, came)
    draws.start()

    def blocks_of(t):
        pair = lists[me, t % n.cap, jnp.bitwise_xor(t // n.cap, me)]
        return pairs[0, pair], pairs[1, pair]

    def copies(i, t):
        both = blocks_of(t)
        return [
            pltpu.make_async_copy(
                matrix.at[:, pl.ds(pl.multiple_of(both[side] * n.width, n.width), n.width)],
                held.at[i, side],
                arrive.at[i],
            )
            for side in range(2)
        ]

    found = list_live(n, 0, last, live, counts)

    def begin(i, carry):
        for copy in copies(i, live[i]):
            copy.start()
        return carry

    lax.fori_loop(0, found, begin, 0)
    clear(outs, n, last * n.part)
    draws.wait()

    def group(i, carry):
        at = [jnp.where(i * unroll + u < found, i * unroll + u, 0) for u in range(unroll)]
        slots = [live[a] for a in at]
        for u in range(unroll):

            @pl.when(i * unroll + u < found)
            def _(u=u):
                for copy in copies(at[u], slots[u]):
                    copy.wait()

        def loads(u, t):
            return held[at[u], 0], held[at[u], 1]

        multiply(n, 0, slots, loads, drawn, blocks_of, stage, outs)
        return carry

    lax.fori_loop(0, pl.cdiv(found, unroll), group, 0)


def late_kernel(n, first, lists, counts, pairs, samples, matrix, after, *rest):
    outs = split_outs(n, rest[: 1 + n.grp_axis // 2])
    sums, stage, live = rest[1 + n.grp_axis // 2 :]
    me = lax.axis_index("rows")
    g = lax.axis_index("grp")
    tile_rows = (n.cap - first) * n.part
    found = list_live(n, first, n.cap, live, counts)
    clear(outs, n, tile_rows)

    def columns(b):
        return matrix[:, pl.ds(pl.multiple_of(b * n.width, n.width), n.width)]

    def block_sum(b, carry):
        x = columns(b).astype(jnp.float32)
        sums[pl.ds(b, 1), :] = jnp.sum(x * x, axis=0, keepdims=True)
        return carry

    lax.fori_loop(0, n.blocks, block_sum, 0, unroll=4)

    for d in range(n.grp_axis):

        def place(o, carry, d=d):
            base = (jnp.bitwise_xor(o, me) * n.grp_axis + jnp.bitwise_xor(g, d)) * n.own
            for j in range(n.own):
                for side in range(2):
                    b = pairs[side, base + j]
                    outs[d][o, pl.ds(tile_rows + 2 * j + side, 1), :] = sums[pl.ds(b, 1), :]
            return carry

        lax.fori_loop(0, n.rows_axis, place, 0)

    def blocks_of(t):
        pair = lists[me, t % n.cap, jnp.bitwise_xor(t // n.cap, me)]
        return pairs[0, pair], pairs[1, pair]

    def group(i, carry):
        slots = [live[jnp.where(i * unroll + u < found, i * unroll + u, 0)] for u in range(unroll)]

        def loads(u, t):
            both = blocks_of(t)
            return columns(both[0]), columns(both[1])

        multiply(n, first, slots, loads, samples.at[0], blocks_of, stage, outs)
        return carry

    lax.fori_loop(0, pl.cdiv(found, unroll), group, 0)


def spread_kernel(n, *refs):
    halves = [refs[:3], refs[3:6]]
    outs = refs[6:]
    for o in range(n.rows_axis):
        at = 0
        for kept, core, chip in halves:
            rows = kept.shape[1]
            outs[o][pl.ds(at, rows), :] = kept[o] + core[0, o] + chip[o]
            at += rows


def gather_kernel(n, lists, *refs):
    parts = refs[: n.rows_axis]
    outs = refs[n.rows_axis : n.rows_axis + n.grp_axis]
    total, acc = refs[n.rows_axis + n.grp_axis :]
    me = lax.axis_index("rows")
    g = lax.axis_index("grp")
    acc[...] = jnp.zeros_like(acc)
    column = jnp.zeros((2 * n.own, n.width), jnp.float32)
    for o in range(n.rows_axis):
        source = jnp.bitwise_xor(me, o)
        for k in range(n.cap):
            i = lists[source, k, me] - me * n.region
            acc[i] += parts[o][pl.ds(k * n.part, n.part), :]
        column = column + parts[o][pl.ds(n.cap * n.part, 2 * n.own), :]
    total[...] = column
    for d in range(n.grp_axis):
        outs[d][...] = acc[pl.ds(jnp.bitwise_xor(g, d) * n.own, n.own)]


def factor_kernel(n, total, out):
    root = jnp.sqrt(total[...] / n.rows_total + epsilon)
    for j in range(n.own):
        left = jnp.transpose(jnp.broadcast_to(root[2 * j : 2 * j + 1], (n.width, n.width)))
        out[j] = 1.0 / (n.samples * left * root[2 * j + 1 : 2 * j + 2])


def scale_kernel(n, factor, *refs):
    parts = refs[: n.grp_axis]
    out = refs[n.grp_axis]
    g = lax.axis_index("grp")
    for d in range(n.grp_axis):
        q = pl.ds(pl.multiple_of(jnp.bitwise_xor(g, d) * n.part, n.part), n.part)
        for j in range(n.own):
            out[j, q, :] = parts[d][j] * factor[j, q, :]


def swap(x, axis, size, distance):
    return lax.ppermute(x, axis, [(i, i ^ distance) for i in range(size)])


def megabytes(*shapes):
    total = sum(4 * functools.reduce(lambda a, b: a * b, s) for s in shapes)
    return pltpu.CompilerParams(vmem_limit_bytes=int(total) + (2 << 20))


def shards(mesh, matrix, sample_rows, pair_list, pair_count, pair_blocks):
    n = Dims(mesh, matrix, sample_rows, pair_list, pair_blocks)
    f32 = jnp.float32
    vmem = pl.BlockSpec(memory_space=pltpu.VMEM)
    smem = pl.BlockSpec(memory_space=pltpu.SMEM)
    hbm = pl.BlockSpec(memory_space=pl.ANY)
    stay = functools.partial(pltpu.with_memory_space_constraint, memory_space=pltpu.HBM)
    lists = stay(jnp.transpose(pair_list, (0, 2, 1)))
    pairs = stay(jnp.transpose(pair_blocks))
    pair_count = stay(pair_count)
    half = n.grp_axis // 2
    first = n.cap - late_slots

    def stage_outs(rows):
        one = (n.rows_axis, rows, n.width)
        return [jax.ShapeDtypeStruct((half,) + one, f32)] + [jax.ShapeDtypeStruct(one, f32)] * half

    stage = (unroll, n.width, n.width)
    slots = n.rows_axis * first
    rows = first * n.part
    early = pl.pallas_call(
        functools.partial(early_kernel, n, first),
        out_shape=stage_outs(rows),
        in_specs=[smem, smem, smem, hbm, hbm],
        out_specs=[vmem] * (1 + half),
        scratch_shapes=[
            pltpu.VMEM((slots, 2, n.rows_dev, n.width), matrix.dtype),
            pltpu.VMEM(sample_rows.shape[1:], jnp.int32),
            pltpu.VMEM(stage, f32),
            pltpu.SMEM((slots,), jnp.int32),
            pltpu.SemaphoreType.DMA((slots,)),
            pltpu.SemaphoreType.DMA,
        ],
        compiler_params=megabytes(
            (slots, n.rows_dev, n.width), stage, sample_rows.shape, (n.grp_axis, n.rows_axis, rows, n.width)
        ),
        name="early_tiles",
    )(lists, pair_count, pairs, stay(sample_rows), stay(matrix))

    def reduce_scatter(outs):
        got = swap(outs[0], "grp", n.grp_axis, 1)
        kept = {2 * i: outs[1 + i] + got[i] for i in range(1, half)}
        sent = kept[half]
        result = [outs[1], got]
        distance = 2
        while distance < n.grp_axis:
            came = {d: swap(kept[d], "grp", n.grp_axis, distance) for d in kept if d & distance}
            result.append(came.pop(distance))
            kept = {d: kept[d] + came[d + distance] for d in kept if not d & distance}
            distance *= 2
        chips = result[2]
        for more in result[3:]:
            chips = chips + more
        return [outs[1], got, chips], sent

    early_sums, sent = reduce_scatter(early)
    late_rows = late_slots * n.part + 2 * n.own
    slots = n.rows_axis * late_slots
    late = pl.pallas_call(
        functools.partial(late_kernel, n, first),
        out_shape=stage_outs(late_rows),
        in_specs=[smem, smem, smem, vmem, vmem, hbm],
        out_specs=[vmem] * (1 + half),
        scratch_shapes=[
            pltpu.VMEM((n.blocks, n.width), f32),
            pltpu.VMEM(stage, f32),
            pltpu.SMEM((slots,), jnp.int32),
        ],
        compiler_params=megabytes(
            stage, (n.blocks, n.width), sample_rows.shape, (n.grp_axis, n.rows_axis, late_rows, n.width)
        ),
        cost_estimate=pl.CostEstimate(
            flops=2 * slots * n.rows_dev * n.width * (n.width + n.samples) + 3 * matrix.size,
            transcendentals=0,
            bytes_accessed=2 * matrix.size,
        ),
        name="late_tiles",
    )(lists, pair_count, pairs, sample_rows, matrix, sent)

    halves = early_sums + reduce_scatter(late)[0]
    message = (n.cap * n.part + 2 * n.own, n.width)
    small = megabytes((4 * n.rows_axis,) + message)
    spread = pl.pallas_call(
        functools.partial(spread_kernel, n),
        out_shape=[jax.ShapeDtypeStruct(message, f32)] * n.rows_axis,
        in_specs=[vmem] * 6,
        out_specs=[vmem] * n.rows_axis,
        compiler_params=small,
        name="spread",
    )(*halves)
    came = [spread[0]]
    for o in range(1, n.rows_axis):
        came.append(swap(spread[o], "rows", n.rows_axis, o))
    quarter = (n.own, n.part, n.width)
    *owned, total = pl.pallas_call(
        functools.partial(gather_kernel, n),
        out_shape=[jax.ShapeDtypeStruct(quarter, f32)] * n.grp_axis
        + [jax.ShapeDtypeStruct((2 * n.own, n.width), f32)],
        in_specs=[smem] + [vmem] * n.rows_axis,
        out_specs=[vmem] * (n.grp_axis + 1),
        scratch_shapes=[pltpu.VMEM((n.region, n.part, n.width), f32)],
        compiler_params=megabytes((n.rows_axis,) + message, (2 * n.grp_axis,) + quarter),
        name="gather",
    )(lists, *came)
    came = [owned[0]] + [
        swap(owned[d], "grp", n.grp_axis, d) for d in reversed(range(1, n.grp_axis))
    ][::-1]
    tiles = (n.own, n.width, n.width)
    factor = pl.pallas_call(
        functools.partial(factor_kernel, n),
        out_shape=jax.ShapeDtypeStruct(tiles, f32),
        in_specs=[vmem],
        out_specs=vmem,
        compiler_params=megabytes(tiles),
        name="factor",
    )(total)
    return pl.pallas_call(
        functools.partial(scale_kernel, n),
        out_shape=jax.ShapeDtypeStruct(tiles, f32),
        in_specs=[vmem] * (n.grp_axis + 1),
        out_specs=vmem,
        compiler_params=megabytes(tiles, tiles, tiles),
        name="scale",
    )(factor, *came)


def solution(mesh):
    in_specs = (P(("rows", "grp"), None), P(("rows", "grp"), None, None), P(), P(), P())
    out_specs = P(("rows", "grp"), None, None)

    def body(*args):
        return shards(mesh, *args)

    return jax.shard_map(body, mesh=mesh, in_specs=in_specs, out_specs=out_specs, check_vma=False)
```

```python
import functools

import jax
import jax.numpy as jnp
from jax import lax
from jax.experimental import pallas as pl
from jax.experimental.pallas import tpu as pltpu
from jax.sharding import PartitionSpec as P

epsilon = 1e-06
unroll = 4
late_slots = 1


class Dims:
    def __init__(self, mesh, matrix, sample_rows, pair_list, pair_blocks):
        self.rows_axis = mesh.shape["rows"]
        self.grp_axis = mesh.shape["grp"]
        self.rows_dev, self.columns = matrix.shape
        self.blocks = sample_rows.shape[1]
        self.samples = sample_rows.shape[2]
        self.width = self.columns // self.blocks
        self.cap = pair_list.shape[2]
        self.pairs = pair_blocks.shape[0]
        self.region = self.pairs // self.rows_axis
        self.own = self.region // self.grp_axis
        self.part = self.width // self.grp_axis
        self.rows_total = self.rows_dev * self.rows_axis * self.grp_axis


def list_live(n, first, last, live, lists, counts, pairs, each=None):
    me = lax.axis_index("rows")

    def scan(o, found):
        r = jnp.bitwise_xor(o, me)
        top = jnp.minimum(counts[me, r], last)
        for k in range(first, last):

            @pl.when(k < top)
            def _(k=k):
                at = found + (k - first)
                pair = lists[me, k, r]
                live[0, at] = o * n.cap + k
                live[1, at] = pairs[0, pair]
                live[2, at] = pairs[1, pair]
                if each is not None:
                    each(at, pairs[0, pair], pairs[1, pair])

        return found + jnp.maximum(top - first, 0)

    return lax.fori_loop(0, n.rows_axis, scan, 0)


def multiply(n, first, at, live, loads, samples, stage, outs):
    g = lax.axis_index("grp")
    positions = lax.broadcasted_iota(jnp.int32, (n.rows_dev, n.samples), 0)
    for u in range(unroll):
        drawn = samples[pl.ds(live[1, at[u]], 1), :]
        times = jnp.sum(jnp.where(drawn == positions, 1.0, 0.0), axis=1, keepdims=True)
        left, right = loads(at[u])
        weighted = (times * left.astype(jnp.float32)).astype(jnp.bfloat16)
        stage[u] = lax.dot_general(
            weighted, right, (((0,), (0,)), ((), ())), preferred_element_type=jnp.float32
        )
    slots = [live[0, a] for a in at]
    for u, t in enumerate(slots):
        o = t // n.cap
        row = pl.multiple_of((t % n.cap - first) * n.part, n.part)
        for d in range(n.grp_axis):
            q = pl.multiple_of(jnp.bitwise_xor(g, d) * n.part, n.part)
            outs[d][o, pl.ds(row, n.part), :] = stage[u, pl.ds(q, n.part), :]


def split_outs(n, refs):
    return [refs[0].at[d // 2] if d % 2 else refs[1 + d // 2] for d in range(n.grp_axis)]


def clear(outs, n, rows):
    zero = jnp.zeros((rows, n.width), jnp.float32)

    def body(o, carry):
        for out in outs:
            out[o, pl.ds(0, rows), :] = zero
        return carry

    lax.fori_loop(0, n.rows_axis, body, 0)


def early_kernel(n, last, lists, counts, pairs, samples, matrix, *rest):
    outs = split_outs(n, rest[: 1 + n.grp_axis // 2])
    held, drawn, stage, live, arrive, came = rest[1 + n.grp_axis // 2 :]
    draws = pltpu.make_async_copy(samples.at[0], drawn, came)
    draws.start()

    def copies(i, b, c):
        return [
            pltpu.make_async_copy(
                matrix.at[:, pl.ds(pl.multiple_of(block * n.width, n.width), n.width)],
                held.at[i, side],
                arrive.at[i],
            )
            for side, block in enumerate((b, c))
        ]

    def begin(i, b, c):
        for copy in copies(i, b, c):
            copy.start()

    found = list_live(n, 0, last, live, lists, counts, pairs, begin)
    clear(outs, n, last * n.part)
    draws.wait()

    def group(i, carry):
        at = [jnp.where(i * unroll + u < found, i * unroll + u, 0) for u in range(unroll)]
        for u in range(unroll):

            @pl.when(i * unroll + u < found)
            def _(u=u):
                for copy in copies(at[u], live[1, at[u]], live[2, at[u]]):
                    copy.wait()

        multiply(n, 0, at, live, lambda a: (held[a, 0], held[a, 1]), drawn, stage, outs)
        return carry

    lax.fori_loop(0, pl.cdiv(found, unroll), group, 0)


def late_kernel(n, first, lists, counts, pairs, samples, matrix, after, *rest):
    outs = split_outs(n, rest[: 1 + n.grp_axis // 2])
    sums, stage, live = rest[1 + n.grp_axis // 2 :]
    me = lax.axis_index("rows")
    g = lax.axis_index("grp")
    tile_rows = (n.cap - first) * n.part
    found = list_live(n, first, n.cap, live, lists, counts, pairs)
    clear(outs, n, tile_rows)

    def columns(b):
        return matrix[:, pl.ds(pl.multiple_of(b * n.width, n.width), n.width)]

    def block_sum(b, carry):
        x = columns(b).astype(jnp.float32)
        sums[pl.ds(b, 1), :] = jnp.sum(x * x, axis=0, keepdims=True)
        return carry

    lax.fori_loop(0, n.blocks, block_sum, 0, unroll=8)

    for d in range(n.grp_axis):

        def place(o, carry, d=d):
            base = (jnp.bitwise_xor(o, me) * n.grp_axis + jnp.bitwise_xor(g, d)) * n.own
            for j in range(n.own):
                for side in range(2):
                    b = pairs[side, base + j]
                    outs[d][o, pl.ds(tile_rows + 2 * j + side, 1), :] = sums[pl.ds(b, 1), :]
            return carry

        lax.fori_loop(0, n.rows_axis, place, 0)

    def group(i, carry):
        at = [jnp.where(i * unroll + u < found, i * unroll + u, 0) for u in range(unroll)]

        def loads(a):
            return columns(live[1, a]), columns(live[2, a])

        multiply(n, first, at, live, loads, samples.at[0], stage, outs)
        return carry

    lax.fori_loop(0, pl.cdiv(found, unroll), group, 0)


def spread_kernel(n, *refs):
    halves = [refs[:3], refs[3:6]]
    outs = refs[6:]
    for o in range(n.rows_axis):
        at = 0
        for kept, core, chip in halves:
            rows = kept.shape[1]
            outs[o][pl.ds(at, rows), :] = kept[o] + core[0, o] + chip[o]
            at += rows


def gather_kernel(n, lists, *refs):
    parts = refs[: n.rows_axis]
    outs = refs[n.rows_axis : n.rows_axis + n.grp_axis]
    total, acc = refs[n.rows_axis + n.grp_axis :]
    me = lax.axis_index("rows")
    g = lax.axis_index("grp")
    acc[...] = jnp.zeros_like(acc)
    column = jnp.zeros((2 * n.own, n.width), jnp.float32)
    for o in range(n.rows_axis):
        source = jnp.bitwise_xor(me, o)
        for k in range(n.cap):
            i = lists[source, k, me] - me * n.region
            acc[i] += parts[o][pl.ds(k * n.part, n.part), :]
        column = column + parts[o][pl.ds(n.cap * n.part, 2 * n.own), :]
    total[...] = column
    for d in range(n.grp_axis):
        outs[d][...] = acc[pl.ds(jnp.bitwise_xor(g, d) * n.own, n.own)]


def factor_kernel(n, total, out):
    root = jnp.sqrt(total[...] / n.rows_total + epsilon)
    for j in range(n.own):
        left = jnp.transpose(jnp.broadcast_to(root[2 * j : 2 * j + 1], (n.width, n.width)))
        out[j] = 1.0 / (n.samples * left * root[2 * j + 1 : 2 * j + 2])


def scale_kernel(n, factor, *refs):
    parts = refs[: n.grp_axis]
    out = refs[n.grp_axis]
    g = lax.axis_index("grp")
    for d in range(n.grp_axis):
        q = pl.ds(pl.multiple_of(jnp.bitwise_xor(g, d) * n.part, n.part), n.part)
        for j in range(n.own):
            out[j, q, :] = parts[d][j] * factor[j, q, :]


def swap(x, axis, size, distance):
    return lax.ppermute(x, axis, [(i, i ^ distance) for i in range(size)])


def megabytes(*shapes):
    total = sum(4 * functools.reduce(lambda a, b: a * b, s) for s in shapes)
    return pltpu.CompilerParams(vmem_limit_bytes=int(total) + (2 << 20))


def shards(mesh, matrix, sample_rows, pair_list, pair_count, pair_blocks):
    n = Dims(mesh, matrix, sample_rows, pair_list, pair_blocks)
    f32 = jnp.float32
    vmem = pl.BlockSpec(memory_space=pltpu.VMEM)
    smem = pl.BlockSpec(memory_space=pltpu.SMEM)
    hbm = pl.BlockSpec(memory_space=pl.ANY)
    stay = functools.partial(pltpu.with_memory_space_constraint, memory_space=pltpu.HBM)
    lists = stay(jnp.transpose(pair_list, (0, 2, 1)))
    pairs = stay(jnp.transpose(pair_blocks))
    pair_count = stay(pair_count)
    half = n.grp_axis // 2
    first = n.cap - late_slots

    def stage_outs(rows):
        one = (n.rows_axis, rows, n.width)
        return [jax.ShapeDtypeStruct((half,) + one, f32)] + [jax.ShapeDtypeStruct(one, f32)] * half

    stage = (unroll, n.width, n.width)
    slots = n.rows_axis * first
    rows = first * n.part
    early = pl.pallas_call(
        functools.partial(early_kernel, n, first),
        out_shape=stage_outs(rows),
        in_specs=[smem, smem, smem, hbm, hbm],
        out_specs=[vmem] * (1 + half),
        scratch_shapes=[
            pltpu.VMEM((slots, 2, n.rows_dev, n.width), matrix.dtype),
            pltpu.VMEM(sample_rows.shape[1:], jnp.int32),
            pltpu.VMEM(stage, f32),
            pltpu.SMEM((3, slots), jnp.int32),
            pltpu.SemaphoreType.DMA((slots,)),
            pltpu.SemaphoreType.DMA,
        ],
        compiler_params=megabytes(
            (slots, n.rows_dev, n.width), stage, sample_rows.shape, (n.grp_axis, n.rows_axis, rows, n.width)
        ),
        name="early_tiles",
    )(lists, pair_count, pairs, stay(sample_rows), stay(matrix))

    def reduce_scatter(outs):
        got = swap(outs[0], "grp", n.grp_axis, 1)
        kept = {2 * i: outs[1 + i] + got[i] for i in range(1, half)}
        sent = kept[half]
        result = [outs[1], got]
        distance = 2
        while distance < n.grp_axis:
            came = {d: swap(kept[d], "grp", n.grp_axis, distance) for d in kept if d & distance}
            result.append(came.pop(distance))
            kept = {d: kept[d] + came[d + distance] for d in kept if not d & distance}
            distance *= 2
        chips = result[2]
        for more in result[3:]:
            chips = chips + more
        return [outs[1], got, chips], sent

    early_sums, sent = reduce_scatter(early)
    late_rows = late_slots * n.part + 2 * n.own
    slots = n.rows_axis * late_slots
    late = pl.pallas_call(
        functools.partial(late_kernel, n, first),
        out_shape=stage_outs(late_rows),
        in_specs=[smem, smem, smem, vmem, vmem, hbm],
        out_specs=[vmem] * (1 + half),
        scratch_shapes=[
            pltpu.VMEM((n.blocks, n.width), f32),
            pltpu.VMEM(stage, f32),
            pltpu.SMEM((3, slots), jnp.int32),
        ],
        compiler_params=megabytes(
            stage, (n.blocks, n.width), sample_rows.shape, (n.grp_axis, n.rows_axis, late_rows, n.width)
        ),
        cost_estimate=pl.CostEstimate(
            flops=2 * slots * n.rows_dev * n.width * (n.width + n.samples) + 3 * matrix.size,
            transcendentals=0,
            bytes_accessed=2 * matrix.size,
        ),
        name="late_tiles",
    )(lists, pair_count, pairs, sample_rows, matrix, sent)

    halves = early_sums + reduce_scatter(late)[0]
    message = (n.cap * n.part + 2 * n.own, n.width)
    small = megabytes((4 * n.rows_axis,) + message)
    spread = pl.pallas_call(
        functools.partial(spread_kernel, n),
        out_shape=[jax.ShapeDtypeStruct(message, f32)] * n.rows_axis,
        in_specs=[vmem] * 6,
        out_specs=[vmem] * n.rows_axis,
        compiler_params=small,
        name="spread",
    )(*halves)
    came = [spread[0]]
    for o in range(1, n.rows_axis):
        came.append(swap(spread[o], "rows", n.rows_axis, o))
    quarter = (n.own, n.part, n.width)
    *owned, total = pl.pallas_call(
        functools.partial(gather_kernel, n),
        out_shape=[jax.ShapeDtypeStruct(quarter, f32)] * n.grp_axis
        + [jax.ShapeDtypeStruct((2 * n.own, n.width), f32)],
        in_specs=[smem] + [vmem] * n.rows_axis,
        out_specs=[vmem] * (n.grp_axis + 1),
        scratch_shapes=[pltpu.VMEM((n.region, n.part, n.width), f32)],
        compiler_params=megabytes((n.rows_axis,) + message, (2 * n.grp_axis,) + quarter),
        name="gather",
    )(jnp.transpose(pair_list, (0, 2, 1)), *came)
    came = [owned[0]]
    for d in range(1, n.grp_axis):
        came.append(swap(owned[d], "grp", n.grp_axis, d))
    tiles = (n.own, n.width, n.width)
    factor = pl.pallas_call(
        functools.partial(factor_kernel, n),
        out_shape=jax.ShapeDtypeStruct(tiles, f32),
        in_specs=[vmem],
        out_specs=vmem,
        compiler_params=megabytes(tiles),
        name="factor",
    )(total)
    return pl.pallas_call(
        functools.partial(scale_kernel, n),
        out_shape=jax.ShapeDtypeStruct(tiles, f32),
        in_specs=[vmem] * (n.grp_axis + 1),
        out_specs=vmem,
        compiler_params=megabytes(tiles, tiles, tiles),
        name="scale",
    )(factor, *came)


def solution(mesh):
    in_specs = (P(("rows", "grp"), None), P(("rows", "grp"), None, None), P(), P(), P())
    out_specs = P(("rows", "grp"), None, None)

    def body(*args):
        return shards(mesh, *args)

    return jax.shard_map(body, mesh=mesh, in_specs=in_specs, out_specs=out_specs, check_vma=False)
```

```python
import functools

import jax
import jax.numpy as jnp
from jax import lax
from jax.experimental import pallas as pl
from jax.experimental.pallas import tpu as pltpu
from jax.sharding import PartitionSpec as P

epsilon = 1e-06
unroll = 4
late_slots = 1
ahead_count = 2


class Dims:
    def __init__(self, mesh, matrix, sample_rows, pair_list, pair_blocks):
        self.rows_axis = mesh.shape["rows"]
        self.grp_axis = mesh.shape["grp"]
        self.rows_dev, self.columns = matrix.shape
        self.blocks = sample_rows.shape[1]
        self.samples = sample_rows.shape[2]
        self.width = self.columns // self.blocks
        self.cap = pair_list.shape[2]
        self.pairs = pair_blocks.shape[0]
        self.region = self.pairs // self.rows_axis
        self.own = self.region // self.grp_axis
        self.part = self.width // self.grp_axis
        self.rows_total = self.rows_dev * self.rows_axis * self.grp_axis


def list_live(n, first, last, live, lists, counts, pairs, each=None):
    me = lax.axis_index("rows")

    def scan(o, found):
        r = jnp.bitwise_xor(o, me)
        top = jnp.minimum(counts[me, r], last)
        for k in range(first, last):

            @pl.when(k < top)
            def _(k=k):
                at = found + (k - first)
                pair = lists[me, k, r]
                live[0, at] = o * n.cap + k
                live[1, at] = pairs[0, pair]
                live[2, at] = pairs[1, pair]
                if each is not None:
                    each(at, pairs[0, pair], pairs[1, pair])

        return found + jnp.maximum(top - first, 0)

    return lax.fori_loop(0, n.rows_axis, scan, 0)


def multiply(n, first, at, live, loads, samples, stage, outs):
    g = lax.axis_index("grp")
    positions = lax.broadcasted_iota(jnp.int32, (n.rows_dev, n.samples), 0)
    for u in range(unroll):
        drawn = samples[pl.ds(live[1, at[u]], 1), :]
        times = jnp.sum(jnp.where(drawn == positions, 1.0, 0.0), axis=1, keepdims=True)
        left, right = loads(at[u])
        weighted = (times * left.astype(jnp.float32)).astype(jnp.bfloat16)
        stage[u] = lax.dot_general(
            weighted, right, (((0,), (0,)), ((), ())), preferred_element_type=jnp.float32
        )
    slots = [live[0, a] for a in at]
    for u, t in enumerate(slots):
        o = t // n.cap
        row = pl.multiple_of((t % n.cap - first) * n.part, n.part)
        for d in range(n.grp_axis):
            q = pl.multiple_of(jnp.bitwise_xor(g, d) * n.part, n.part)
            outs[d][o, pl.ds(row, n.part), :] = stage[u, pl.ds(q, n.part), :]


def split_outs(n, refs):
    return [refs[0].at[d // 2] if d % 2 else refs[1 + d // 2] for d in range(n.grp_axis)]


def clear(outs, n, rows):
    zero = jnp.zeros((rows, n.width), jnp.float32)

    def body(o, carry):
        for out in outs:
            out[o, pl.ds(0, rows), :] = zero
        return carry

    lax.fori_loop(0, n.rows_axis, body, 0)


def early_kernel(n, last, lists, counts, pairs, samples, matrix, *rest):
    outs = split_outs(n, rest[: 1 + n.grp_axis // 2])
    held, drawn, stage, live, arrive, came = rest[1 + n.grp_axis // 2 :]
    draws = pltpu.make_async_copy(samples.at[0], drawn, came)
    draws.start()

    def copies(i, b, c):
        return [
            pltpu.make_async_copy(
                matrix.at[:, pl.ds(pl.multiple_of(block * n.width, n.width), n.width)],
                held.at[i, side],
                arrive.at[i],
            )
            for side, block in enumerate((b, c))
        ]

    def begin(i, b, c):
        for copy in copies(i, b, c):
            copy.start()

    found = list_live(n, 0, last, live, lists, counts, pairs, begin)
    clear(outs, n, last * n.part)
    draws.wait()

    def group(i, carry):
        at = [jnp.where(i * unroll + u < found, i * unroll + u, 0) for u in range(unroll)]
        for u in range(unroll):

            @pl.when(i * unroll + u < found)
            def _(u=u):
                for copy in copies(at[u], live[1, at[u]], live[2, at[u]]):
                    copy.wait()

        multiply(n, 0, at, live, lambda a: (held[a, 0], held[a, 1]), drawn, stage, outs)
        return carry

    lax.fori_loop(0, pl.cdiv(found, unroll), group, 0)


def late_kernel(n, first, lists, counts, pairs, samples, matrix, after, *rest):
    outs = split_outs(n, rest[: 1 + n.grp_axis // 2])
    sums, stage, live = rest[1 + n.grp_axis // 2 :]
    me = lax.axis_index("rows")
    g = lax.axis_index("grp")
    tile_rows = (n.cap - first) * n.part
    found = list_live(n, first, n.cap, live, lists, counts, pairs)
    clear(outs, n, tile_rows)

    def columns(b):
        return matrix[:, pl.ds(pl.multiple_of(b * n.width, n.width), n.width)]

    def block_sum(b, carry):
        x = columns(b).astype(jnp.float32)
        sums[pl.ds(b, 1), :] = jnp.sum(x * x, axis=0, keepdims=True)
        return carry

    lax.fori_loop(0, n.blocks, block_sum, 0, unroll=8)

    for d in range(n.grp_axis):

        def place(o, carry, d=d):
            base = (jnp.bitwise_xor(o, me) * n.grp_axis + jnp.bitwise_xor(g, d)) * n.own
            for j in range(n.own):
                for side in range(2):
                    b = pairs[side, base + j]
                    outs[d][o, pl.ds(tile_rows + 2 * j + side, 1), :] = sums[pl.ds(b, 1), :]
            return carry

        lax.fori_loop(0, n.rows_axis, place, 0)

    def group(i, carry):
        at = [jnp.where(i * unroll + u < found, i * unroll + u, 0) for u in range(unroll)]

        def loads(a):
            return columns(live[1, a]), columns(live[2, a])

        multiply(n, first, at, live, loads, samples.at[0], stage, outs)
        return carry

    lax.fori_loop(0, pl.cdiv(found, unroll), group, 0)


def ahead(n):
    return range(n.rows_axis // 2, min(n.rows_axis // 2 + ahead_count, n.rows_axis))


def ahead_kernel(n, kept, core, chip, *outs):
    for out, o in zip(outs, ahead(n)):
        out[...] = kept[o] + core[0, o] + chip[o]


def spread_kernel(n, *refs):
    chunks = [refs[:3], refs[3:6]]
    outs = refs[6:]
    for o in range(n.rows_axis):
        at = 0
        for kept, core, chip in chunks[o in ahead(n) :]:
            rows = kept.shape[1]
            outs[o][pl.ds(at, rows), :] = kept[o] + core[0, o] + chip[o]
            at += rows


def gather_kernel(n, first, lists, *refs):
    parts = refs[: n.rows_axis]
    early = dict(zip(ahead(n), refs[n.rows_axis : n.rows_axis + len(ahead(n))]))
    refs = refs[n.rows_axis + len(ahead(n)) :]
    outs = refs[: n.grp_axis]
    total, acc = refs[n.grp_axis :]
    me = lax.axis_index("rows")
    g = lax.axis_index("grp")
    acc[...] = jnp.zeros_like(acc)
    column = jnp.zeros((2 * n.own, n.width), jnp.float32)
    for o in range(n.rows_axis):
        source = jnp.bitwise_xor(me, o)
        skipped = first if o in early else 0
        for k in range(n.cap):
            i = lists[source, k, me] - me * n.region
            part, at = (early[o], k) if k < skipped else (parts[o], k - skipped)
            acc[i] += part[pl.ds(at * n.part, n.part), :]
        column = column + parts[o][pl.ds((n.cap - skipped) * n.part, 2 * n.own), :]
    total[...] = column
    for d in range(n.grp_axis):
        outs[d][...] = acc[pl.ds(jnp.bitwise_xor(g, d) * n.own, n.own)]


def factor_kernel(n, total, out):
    root = jnp.sqrt(total[...] / n.rows_total + epsilon)
    for j in range(n.own):
        left = jnp.transpose(jnp.broadcast_to(root[2 * j : 2 * j + 1], (n.width, n.width)))
        out[j] = 1.0 / (n.samples * left * root[2 * j + 1 : 2 * j + 2])


def scale_kernel(n, factor, *refs):
    parts = refs[: n.grp_axis]
    out = refs[n.grp_axis]
    g = lax.axis_index("grp")
    for d in range(n.grp_axis):
        q = pl.ds(pl.multiple_of(jnp.bitwise_xor(g, d) * n.part, n.part), n.part)
        for j in range(n.own):
            out[j, q, :] = parts[d][j] * factor[j, q, :]


def swap(x, axis, size, distance):
    return lax.ppermute(x, axis, [(i, i ^ distance) for i in range(size)])


def megabytes(*shapes):
    total = sum(4 * functools.reduce(lambda a, b: a * b, s) for s in shapes)
    return pltpu.CompilerParams(vmem_limit_bytes=int(total) + (2 << 20))


def shards(mesh, matrix, sample_rows, pair_list, pair_count, pair_blocks):
    n = Dims(mesh, matrix, sample_rows, pair_list, pair_blocks)
    f32 = jnp.float32
    vmem = pl.BlockSpec(memory_space=pltpu.VMEM)
    smem = pl.BlockSpec(memory_space=pltpu.SMEM)
    hbm = pl.BlockSpec(memory_space=pl.ANY)
    stay = functools.partial(pltpu.with_memory_space_constraint, memory_space=pltpu.HBM)
    lists = stay(jnp.transpose(pair_list, (0, 2, 1)))
    pairs = stay(jnp.transpose(pair_blocks))
    pair_count = stay(pair_count)
    half = n.grp_axis // 2
    first = n.cap - late_slots

    def stage_outs(rows):
        one = (n.rows_axis, rows, n.width)
        return [jax.ShapeDtypeStruct((half,) + one, f32)] + [jax.ShapeDtypeStruct(one, f32)] * half

    stage = (unroll, n.width, n.width)
    slots = n.rows_axis * first
    rows = first * n.part
    early = pl.pallas_call(
        functools.partial(early_kernel, n, first),
        out_shape=stage_outs(rows),
        in_specs=[smem, smem, smem, hbm, hbm],
        out_specs=[vmem] * (1 + half),
        scratch_shapes=[
            pltpu.VMEM((slots, 2, n.rows_dev, n.width), matrix.dtype),
            pltpu.VMEM(sample_rows.shape[1:], jnp.int32),
            pltpu.VMEM(stage, f32),
            pltpu.SMEM((3, slots), jnp.int32),
            pltpu.SemaphoreType.DMA((slots,)),
            pltpu.SemaphoreType.DMA,
        ],
        compiler_params=megabytes(
            (slots, n.rows_dev, n.width), stage, sample_rows.shape, (n.grp_axis, n.rows_axis, rows, n.width)
        ),
        name="early_tiles",
    )(lists, pair_count, pairs, stay(sample_rows), stay(matrix))

    def reduce_scatter(outs):
        got = swap(outs[0], "grp", n.grp_axis, 1)
        kept = {2 * i: outs[1 + i] + got[i] for i in range(1, half)}
        sent = kept[half]
        result = [outs[1], got]
        distance = 2
        while distance < n.grp_axis:
            came = {d: swap(kept[d], "grp", n.grp_axis, distance) for d in kept if d & distance}
            result.append(came.pop(distance))
            kept = {d: kept[d] + came[d + distance] for d in kept if not d & distance}
            distance *= 2
        chips = result[2]
        for more in result[3:]:
            chips = chips + more
        return [outs[1], got, chips], sent

    early_sums, sent = reduce_scatter(early)
    late_rows = late_slots * n.part + 2 * n.own
    slots = n.rows_axis * late_slots
    late = pl.pallas_call(
        functools.partial(late_kernel, n, first),
        out_shape=stage_outs(late_rows),
        in_specs=[smem, smem, smem, vmem, vmem, hbm],
        out_specs=[vmem] * (1 + half),
        scratch_shapes=[
            pltpu.VMEM((n.blocks, n.width), f32),
            pltpu.VMEM(stage, f32),
            pltpu.SMEM((3, slots), jnp.int32),
        ],
        compiler_params=megabytes(
            stage, (n.blocks, n.width), sample_rows.shape, (n.grp_axis, n.rows_axis, late_rows, n.width)
        ),
        cost_estimate=pl.CostEstimate(
            flops=2 * slots * n.rows_dev * n.width * (n.width + n.samples) + 3 * matrix.size,
            transcendentals=0,
            bytes_accessed=2 * matrix.size,
        ),
        name="late_tiles",
    )(lists, pair_count, pairs, sample_rows, matrix, sent)

    first_rows = (first * n.part, n.width)
    spread_ahead = pl.pallas_call(
        functools.partial(ahead_kernel, n),
        out_shape=[jax.ShapeDtypeStruct(first_rows, f32)] * len(ahead(n)),
        in_specs=[vmem] * 3,
        out_specs=[vmem] * len(ahead(n)),
        compiler_params=megabytes((4 * n.rows_axis,) + first_rows),
        name="ahead",
    )(*early_sums)
    came_ahead = []
    for o, part in zip(ahead(n), spread_ahead):
        came_ahead.append(swap(part, "rows", n.rows_axis, o))
    halves = early_sums + reduce_scatter(late)[0]
    message = (n.cap * n.part + 2 * n.own, n.width)
    shorter = (message[0] - first_rows[0], n.width)
    spread = pl.pallas_call(
        functools.partial(spread_kernel, n),
        out_shape=[
            jax.ShapeDtypeStruct(shorter if o in ahead(n) else message, f32) for o in range(n.rows_axis)
        ],
        in_specs=[vmem] * 6,
        out_specs=[vmem] * n.rows_axis,
        compiler_params=megabytes((4 * n.rows_axis,) + message),
        name="spread",
    )(*halves)
    came = [spread[0]]
    for o in range(1, n.rows_axis):
        came.append(swap(spread[o], "rows", n.rows_axis, o))
    came += came_ahead
    quarter = (n.own, n.part, n.width)
    *owned, total = pl.pallas_call(
        functools.partial(gather_kernel, n, first),
        out_shape=[jax.ShapeDtypeStruct(quarter, f32)] * n.grp_axis
        + [jax.ShapeDtypeStruct((2 * n.own, n.width), f32)],
        in_specs=[smem] + [vmem] * len(came),
        out_specs=[vmem] * (n.grp_axis + 1),
        scratch_shapes=[pltpu.VMEM((n.region, n.part, n.width), f32)],
        compiler_params=megabytes((n.rows_axis,) + message, (2 * n.grp_axis,) + quarter),
        name="gather",
    )(jnp.transpose(pair_list, (0, 2, 1)), *came)
    came = [owned[0]]
    for d in range(1, n.grp_axis):
        came.append(swap(owned[d], "grp", n.grp_axis, d))
    tiles = (n.own, n.width, n.width)
    factor = pl.pallas_call(
        functools.partial(factor_kernel, n),
        out_shape=jax.ShapeDtypeStruct(tiles, f32),
        in_specs=[vmem],
        out_specs=vmem,
        compiler_params=megabytes(tiles),
        name="factor",
    )(total)
    return pl.pallas_call(
        functools.partial(scale_kernel, n),
        out_shape=jax.ShapeDtypeStruct(tiles, f32),
        in_specs=[vmem] * (n.grp_axis + 1),
        out_specs=vmem,
        compiler_params=megabytes(tiles, tiles, tiles),
        name="scale",
    )(factor, *came)


def solution(mesh):
    in_specs = (P(("rows", "grp"), None), P(("rows", "grp"), None, None), P(), P(), P())
    out_specs = P(("rows", "grp"), None, None)

    def body(*args):
        return shards(mesh, *args)

    return jax.shard_map(body, mesh=mesh, in_specs=in_specs, out_specs=out_specs, check_vma=False)
```
